32 devices in a mesh: tok: 4 (over z), hid: 8 (over y, x, core).
Axes of the slice: x: 2, y: 2, z: 4, core: 2. Of those that a mesh axis runs over, the one named last changes fastest.
Arguments:
- tokens: bfloat16 [512, 4096], P('tok', 'hid'), may hold values from -6 to 6
- out_grad: bfloat16 [512, 4096], P('tok', 'hid'), may hold values from -6 to 6
- routing_ids: int32 [512, 2], P('tok'), may hold values from 0 to 3, all different within a row; in each aligned block of 128 rows (0 to 127, 128 to 255, ...) at most 96 rows name the same one
- route_weights: bfloat16 [512, 2], P('tok'), may hold values from 0.049804688 to 1
- gate_matrix: bfloat16 [4, 4096, 8192], P('tok', None, 'hid'), may hold values from -0.125 to 0.125
- up_matrix: bfloat16 [4, 4096, 8192], P('tok', None, 'hid'), may hold values from -0.09375 to 0.09375
- down_matrix: bfloat16 [4, 8192, 4096], P('tok', 'hid'), may hold values from -0.0625 to 0.0625
Outputs:
- input_grad: bfloat16 [512, 4096], P('tok', 'hid')
- route_grad: bfloat16 [512, 2], P('tok')
- gate_matrix_grad: bfloat16 [4, 4096, 8192], P('tok', None, 'hid')
- up_matrix_grad: bfloat16 [4, 4096, 8192], P('tok', None, 'hid')
- down_matrix_grad: bfloat16 [4, 8192, 4096], P('tok', 'hid')
The draws below stay inside these ranges and needn't reach their ends.
Inputs may be any that keep to these rules, and one draw needn't show every extreme that they name: `routing_ids`: each token names two different experts. Among the 128 tokens of one index of tok no expert is named more than 96 times, a bound that some expert reaches in each such block.
All inputs are finite; a program needn't handle non-finite values.
Results may differ from the reference program's by a relative error of at most 0.0076.
Values may be sent and summed in bfloat16 or wider, within the bound.
A program may use at most 128 MiB of HBM per device.

```python
import math
import jax
import jax.numpy as jnp
import numpy as np
from jax import lax

D = 4096
FF = 8192
TOK_DEV = 128
EXPERTS = 4
TOKENS = 512
CAP = 96
N_TOK = 4


def strengthened(drawn, rng, source, target, shards_of, factor):
    def block_of(axis_at):
        return (jnp.arange(drawn.shape[axis_at]) // (drawn.shape[axis_at] // shards_of)).reshape((-1,) + (1,) * (drawn.ndim - 1 - axis_at))

    one_side = jax.random.permutation(rng, shards_of)[block_of(target)]
    second = (block_of(target) + shards_of // 2) % shards_of
    return jnp.where((block_of(source) == one_side) | (block_of(source) == second), factor * drawn, drawn)


def block_levels(key, shape, shards, low, top_value):
    def one(axis_at, shards_of):
        draws = jax.random.uniform(jax.random.fold_in(jax.random.fold_in(key, 6), axis_at), (shards_of,), jnp.float32, low / len(shards), top_value / len(shards))
        return jnp.repeat(jnp.exp(draws), shape[axis_at] // shards_of).reshape((-1,) + (1,) * (len(shape) - axis_at - 1))

    level = one(*shards[0])
    for cut in shards[1:]:
        level = level * one(*cut)
    return level


def deal_out(rng, own, number, rows, count, top, most, skew):
    ranking = jax.random.permutation(rng, count)
    crowded, usual = portions_of(count, rows * top, most, skew, True), portions_of(count, rows * top, most, skew, False)
    places = jnp.arange(count)

    def named(tallies, offset_by):
        used = int((tallies > 0).sum())
        fixed = max(1, used // 4)
        shifted = fixed + (places - fixed + offset_by * (used - fixed)) % max(1, count - fixed)
        return jnp.zeros((count,), jnp.int32).at[ranking[jnp.where(places < fixed, places, shifted)]].set(jnp.asarray(tallies, jnp.int32))

    tallies = jnp.where(number % 4 == 0, named(crowded, number // 4), named(usual, number - number // 4 - 1))
    mixed = jax.random.permutation(jax.random.fold_in(own, 3), count)
    source_of, sink = mixed[0:count // 2 * 2:2], mixed[1:count // 2 * 2:2]
    margin = jnp.minimum(tallies[source_of] - 1, most - tallies[sink]) // 2
    margin = jnp.where((source_of == ranking[0]) | (sink == ranking[0]) | (tallies[sink] == 0), 0, jnp.maximum(margin, 0))
    shifted = jax.random.randint(jax.random.fold_in(own, 4), (count // 2,), 0, 1 << 20) % (margin + 1)
    tallies = tallies.at[source_of].add(-shifted).at[sink].add(shifted)
    members = jnp.searchsorted(jnp.cumsum(tallies), jnp.arange(rows * top), side="right").astype(jnp.int32)
    listing = members.reshape(top, rows).T
    listing = listing[jax.random.permutation(jax.random.fold_in(own, 1), rows)]
    offset_by = jax.random.randint(jax.random.fold_in(own, 2), (rows, 1), 0, top)
    return jnp.take_along_axis(listing, (jnp.arange(top)[None, :] + offset_by) % top, axis=1)


def portions_of(amount, total, limit, lean, full):
    portions = [(1 << 20) // math.isqrt(grade ** lean) + 1 for grade in range(1, amount + 1)]
    largest = limit if full else min(limit, max(-(-total // amount), total * portions[0] // sum(portions)))
    least = 1 if total - largest >= amount - 1 else 0
    given, rest = [largest] + [least] * (amount - 1), total - largest - least * (amount - 1)
    while rest > 0:
        movable = [i for i in range(1, amount) if given[i] < largest] or [i for i in range(1, amount) if given[i] < limit]
        whole, remaining = sum([portions[i] for i in movable]), rest
        for i in movable:
            addition = min(limit - given[i], max(1, remaining * portions[i] // whole), rest)
            given[i] = given[i] + addition
            rest = rest - addition
    return np.array(given)


def gaussian(own_key, dims, deviation, bound, shards=(), held_as=jnp.bfloat16):
    result = deviation * jax.random.normal(own_key, dims, jnp.float32)
    if shards:
        result = result * block_levels(own_key, dims, shards, -0.22, 0.18)
    return jnp.clip(result, -bound, bound).astype(held_as)


def bell_draw_with(own_key, extent, width, limit, split, heavy, kind=jnp.bfloat16):
    values = width * jax.random.normal(own_key, extent, jnp.float32)
    if split:
        values = values * block_levels(own_key, extent, split, -0.22, 0.18)
    return jnp.clip(strengthened(values, jax.random.fold_in(own_key, 3), *heavy), -limit, limit).astype(kind)


def setup_inputs(seed: int = 0) -> dict:
    keys = jax.random.split(jax.random.key(seed), 8)
    tokens = gaussian(keys[0], (TOKENS, D), 1.0, 6.0, ((0, 4), (1, 8)))
    out_grad = gaussian(keys[1], (TOKENS, D), 1.0, 6.0, ((0, 4), (1, 8)))
    routing_ids_keys = jax.random.split(jax.random.fold_in(keys[2], 1), TOKENS // TOK_DEV)
    routing_ids_turns = jax.random.permutation(jax.random.fold_in(keys[2], 3), TOKENS // TOK_DEV)
    routing_ids = jax.vmap(lambda own, number: deal_out(jax.random.fold_in(keys[2], 2), own, number, TOK_DEV, EXPERTS, 2, CAP, 2))(routing_ids_keys, routing_ids_turns).reshape((TOKENS, 2))
    route_weights = jnp.clip(jnp.exp(math.log(1.0) - 2.9996462 * jax.random.uniform(keys[3], (TOKENS, 2), jnp.float32) ** block_levels(keys[3], (TOKENS, 2), ((0, 4),), -0.2, 0.2)), 0.049804688, 1.0).astype(jnp.bfloat16)
    gate_matrix = bell_draw_with(keys[4], (EXPERTS, D, FF), D ** -0.5, 0.125, ((0, 4), (2, 8)), (2, 1, 8, 2.0))
    up_matrix = gaussian(keys[5], (EXPERTS, D, FF), D ** -0.5, 0.09375, ((0, 4), (2, 8)))
    down_matrix = gaussian(keys[6], (EXPERTS, FF, D), FF ** -0.5, 0.0625, ((0, 4), (1, 8)))
    return {"tokens": tokens, "out_grad": out_grad, "routing_ids": routing_ids, "route_weights": route_weights, "gate_matrix": gate_matrix, "up_matrix": up_matrix, "down_matrix": down_matrix}


def contract(left, right, left_dim, right_dim):
    return lax.dot_general(left, right, (((left_dim,), (right_dim,)), ((), ())), preferred_element_type=jnp.float32)


def expert_pass(items):
    rows_in, rows_grad, rows_weight, gate_w, up_w, down_w = items
    gate = contract(rows_in, gate_w, 1, 0)
    upper = contract(rows_in, up_w, 1, 0)
    sig = jax.nn.sigmoid(gate)
    act = gate * sig
    weight_col = rows_weight.astype(jnp.float32)[:, None]
    hidden = (act * upper).astype(jnp.bfloat16)
    scaled = (act * upper * weight_col).astype(jnp.bfloat16)
    back = contract(rows_grad, down_w, 1, 1)
    route_part = jnp.sum(hidden.astype(jnp.float32) * back, axis=1)
    back_scaled = back * weight_col
    up_delta = (back_scaled * act).astype(jnp.bfloat16)
    gate_delta = (back_scaled * upper * sig * (1.0 + gate * (1.0 - sig))).astype(jnp.bfloat16)
    gate_out = contract(rows_in, gate_delta, 0, 0).astype(jnp.bfloat16)
    up_out = contract(rows_in, up_delta, 0, 0).astype(jnp.bfloat16)
    down_out = contract(scaled, rows_grad, 0, 0).astype(jnp.bfloat16)
    row_grads = (contract(gate_delta, gate_w, 1, 1) + contract(up_delta, up_w, 1, 1)).astype(jnp.bfloat16)
    return gate_out, up_out, down_out, row_grads, route_part


def reference(tokens, out_grad, routing_ids, route_weights, gate_matrix, up_matrix, down_matrix):
    blocks = N_TOK
    expert_count = EXPERTS
    flat = routing_ids.reshape(blocks, -1).astype(jnp.int32)
    choices = flat.shape[1]
    onehot = (flat[:, :, None] == jnp.arange(expert_count, dtype=jnp.int32)[None, None, :]).astype(jnp.int32)
    position = jnp.sum((jnp.cumsum(onehot, axis=1) - onehot) * onehot, axis=2)
    block_ids = jnp.arange(blocks, dtype=jnp.int32)[:, None]
    table_row = (flat * (blocks * CAP) + block_ids * CAP + position).reshape(-1).astype(jnp.int32)
    total = blocks * choices
    table_size = expert_count * blocks * CAP
    source = jnp.full((table_size,), total, jnp.int32).at[table_row].set(jnp.arange(total, dtype=jnp.int32))
    valid = source < total
    clipped = jnp.minimum(source, total - 1)
    token_row = clipped // 2
    rows_in = jnp.where(valid[:, None], tokens[token_row], jnp.zeros((), jnp.bfloat16))
    rows_grad = jnp.where(valid[:, None], out_grad[token_row], jnp.zeros((), jnp.bfloat16))
    rows_weight = jnp.where(valid, route_weights.reshape(-1)[clipped], jnp.zeros((), jnp.bfloat16))
    per = blocks * CAP
    gate_out, up_out, down_out, row_grads, route_part = lax.map(
        expert_pass,
        (rows_in.reshape(expert_count, per, -1), rows_grad.reshape(expert_count, per, -1),
         rows_weight.reshape(expert_count, per), gate_matrix, up_matrix, down_matrix))
    row_grads = row_grads.reshape(table_size, -1)
    picked = row_grads[table_row].astype(jnp.float32)
    input_grad = jnp.sum(picked.reshape(total // 2, 2, -1), axis=1).astype(jnp.bfloat16)
    route_grad = route_part.reshape(-1)[table_row].astype(jnp.bfloat16).reshape(total // 2, 2)
    return input_grad, route_grad, gate_out, up_out, down_out
```

```python
import jax
import jax.numpy as jnp
from jax import lax
from jax.experimental import pallas as pl
from jax.experimental.pallas import tpu as pltpu
from jax.sharding import PartitionSpec as P


def flip(index, relative, bits):
    for b in range(bits):
        if (relative >> b) & 1:
            index = index + (1 << b) - 2 * (1 << b) * ((index // (1 << b)) % 2)
    return index


def spread_kernel(bits, count, *refs):
    sources, outs = refs[:count], refs[count:2 * count]
    send, recv, local = refs[2 * count:]
    me = lax.axis_index("hid")
    rows, width = sources[0].shape
    half = rows // 2
    barrier = pltpu.get_barrier_semaphore()
    for b in range(bits):
        pl.semaphore_signal(
            barrier, inc=1, device_id={"hid": flip(me, 1 << b, bits)}, device_id_type=pl.DeviceIdType.MESH
        )
    pl.semaphore_wait(barrier, bits)
    outer = list(range(1, bits))
    orders = (outer + [0], outer[::-1] + [0])

    def columns(block):
        return pl.ds(pl.multiple_of(block * width, width), width)

    own = []
    for a in range(count):
        copy = pltpu.make_async_copy(sources[a], outs[a].at[:, columns(me)], local.at[a])
        copy.start()
        own.append(copy)
    everything, pending = [], {}
    for step in range(bits):
        for a in range(count):
            for h in range(2):
                order = orders[h]
                held = [0]
                for b in order[:step]:
                    held = held + [d ^ (1 << b) for d in held]
                for copy in pending.pop((a, h), []):
                    copy.wait_recv()
                started = []
                partner = flip(me, 1 << order[step], bits)
                lines = pl.ds(h * half, half)
                for d in held:
                    block = flip(me, d, bits)
                    where = outs[a].at[lines, columns(block)]
                    what = sources[a].at[lines, :] if d == 0 else where
                    slot = (a * 2 + h) * (1 << bits) + len(held) + held.index(d)
                    copy = pltpu.make_async_remote_copy(
                        src_ref=what, dst_ref=where, send_sem=send.at[slot], recv_sem=recv.at[slot],
                        device_id={"hid": partner}, device_id_type=pl.DeviceIdType.MESH,
                    )
                    copy.start()
                    started.append(copy)
                pending[(a, h)] = started
                everything += started
    for started in pending.values():
        for copy in started:
            copy.wait_recv()
    for copy in everything:
        copy.wait_send()
    for copy in own:
        copy.wait()


def spread(number, *blocks):
    size = lax.axis_size("hid")
    bits = size.bit_length() - 1
    count = len(blocks)
    rows, width = blocks[0].shape
    whole = pl.BlockSpec(memory_space=pltpu.VMEM)
    slots = 2 * count * size
    return pl.pallas_call(
        lambda *refs: spread_kernel(bits, count, *refs),
        out_shape=[jax.ShapeDtypeStruct((rows, width * size), b.dtype) for b in blocks],
        in_specs=[whole] * count,
        out_specs=[whole] * count,
        scratch_shapes=[
            pltpu.SemaphoreType.DMA((slots,)),
            pltpu.SemaphoreType.DMA((slots,)),
            pltpu.SemaphoreType.DMA((count,)),
        ],
        compiler_params=pltpu.CompilerParams(
            collective_id=number, has_side_effects=True, vmem_limit_bytes=32 * 1024 * 1024
        ),
        cost_estimate=pl.CostEstimate(flops=20_000_000_000, bytes_accessed=4 * rows * width * size * count, transcendentals=0),
    )(*blocks)


def contract(left, right, left_dim, right_dim):
    return lax.dot_general(
        left, right, (((left_dim,), (right_dim,)), ((), ())), preferred_element_type=jnp.float32
    )


def per_device(tokens, out_grad, routing_ids, route_weights, gate_matrix, up_matrix, down_matrix):
    groups = lax.axis_size("tok")
    tok_rows = tokens.shape[0]
    capacity = 3 * tok_rows // groups
    flat = routing_ids.reshape(-1)
    choices = flat.shape[0]
    onehot = (flat[:, None] == jnp.arange(groups, dtype=jnp.int32)[None, :]).astype(jnp.int32)
    position = jnp.sum((jnp.cumsum(onehot, axis=0) - onehot) * onehot, axis=1)
    slots = flat * capacity + position
    table = jnp.arange(groups * capacity, dtype=jnp.int32)
    match = (table[:, None, None] == slots.reshape(tok_rows, 2)[None]).astype(jnp.bfloat16)
    named = match[:, :, 0] + match[:, :, 1]
    slot_weight = jnp.sum(match * route_weights[None], axis=(1, 2), dtype=jnp.float32)
    both = jnp.concatenate([tokens, out_grad], axis=1)
    packed = contract(named, both, 1, 0).astype(jnp.bfloat16)
    width = tokens.shape[1]
    tail = jnp.broadcast_to(slot_weight.astype(jnp.bfloat16)[:, None], (groups * capacity, 128))
    packed = jnp.concatenate([packed, tail], axis=1)
    moved = lax.all_to_all(packed, "tok", split_axis=0, concat_axis=0, tiled=True)
    slice_in, slice_grad, rows_weight = moved[:, :width], moved[:, width:2 * width], moved[:, 2 * width]
    rows_in, rows_grad = spread(1, slice_in, slice_grad)
    gate_w = gate_matrix[0]
    up_w = up_matrix[0]
    down_w = down_matrix[0]
    gate = contract(rows_in, gate_w, 1, 0)
    upper = contract(rows_in, up_w, 1, 0)
    sig = jax.nn.sigmoid(gate)
    act = gate * sig
    weight_col = rows_weight.astype(jnp.float32)[:, None]
    hidden = (act * upper).astype(jnp.bfloat16)
    scaled = (act * upper * weight_col).astype(jnp.bfloat16)
    back = contract(rows_grad, down_w, 1, 1)
    route_local = jnp.sum(hidden.astype(jnp.float32) * back, axis=1)
    back_scaled = back * weight_col
    up_delta = (back_scaled * act).astype(jnp.bfloat16)
    gate_delta = (back_scaled * upper * sig * (1.0 + gate * (1.0 - sig))).astype(jnp.bfloat16)
    gate_out = contract(rows_in, gate_delta, 0, 0).astype(jnp.bfloat16)
    up_out = contract(rows_in, up_delta, 0, 0).astype(jnp.bfloat16)
    down_out = contract(scaled, rows_grad, 0, 0).astype(jnp.bfloat16)
    shares = lax.psum_scatter(
        (contract(gate_w, gate_delta, 1, 1) + contract(up_w, up_delta, 1, 1)).astype(jnp.bfloat16),
        "hid",
        scatter_dimension=0,
        tiled=True,
    )
    route_total = lax.psum(route_local, "hid").astype(jnp.bfloat16)
    moved_back = jnp.concatenate(
        [shares, jnp.broadcast_to(route_total[None], (16, route_total.shape[0]))], axis=0
    )
    back_rows = lax.all_to_all(moved_back, "tok", split_axis=1, concat_axis=1, tiled=True)
    features = tokens.shape[1]
    input_grad = contract(named, back_rows[:features], 0, 1).astype(jnp.bfloat16)
    back_route = back_rows[features].astype(jnp.float32)
    route_grad = jnp.sum(match.astype(jnp.float32) * back_route[:, None, None], axis=0)
    route_grad = route_grad.astype(jnp.bfloat16)
    return (input_grad, route_grad, gate_out[None], up_out[None], down_out[None])


def solution(mesh):
    in_specs = (
        P("tok", "hid"),
        P("tok", "hid"),
        P("tok", None),
        P("tok", None),
        P("tok", None, "hid"),
        P("tok", None, "hid"),
        P("tok", "hid", None),
    )
    out_specs = (
        P("tok", "hid"),
        P("tok", None),
        P("tok", None, "hid"),
        P("tok", None, "hid"),
        P("tok", "hid", None),
    )
    return jax.shard_map(
        per_device, mesh=mesh, in_specs=in_specs, out_specs=out_specs, check_vma=False
    )
```
